32 devices in a mesh: gx: 4 (over z), wa: 8 (over y, x, core).
Axes of the slice: x: 2, y: 2, z: 4, core: 2. Of those that a mesh axis runs over, the one named last changes fastest.
Arguments:
- positions: float32 [512, 3, 256], P(('gx', 'wa')), may hold values from 0 to 1
- weights: float32 [512, 256], P(('gx', 'wa')), may hold values from 0.5 to 2
- block_count: int32 [512], P(('gx', 'wa')), may hold values from 1 to 256
- send_list: int32 [32, 8, 2], P(('gx', 'wa')), may hold values from 0 to 15
- unit_pair: int32 [32, 16], P(('gx', 'wa')), may hold values from 0 to 15, each once within a row
- unit_live: int32 [32], P(('gx', 'wa')), may hold values from 2 to 16, as said below
Outputs:
- slab_counts: float32 [4, 30, 20], P('gx')
- totals: float32 [30, 20], replicated
The draws below stay inside these ranges and needn't reach their ends.
Inputs may be any that keep to these rules, and one draw needn't show every extreme that they name: `unit_pair`: each row holds every slot number once. `unit_live`: the active units of a device are the first ones of its list; some device has all 16 active.
All inputs are finite; a program needn't handle non-finite values.
Results may differ from the reference program's by a relative error of at most 0.0003.
Values sent between devices are 32-bit elements; how exact they have to be, the bound alone decides.
No kernel may reach another device: no remote copies, remote signals or barrier semaphores. Data moves between devices by JAX's collectives and lax.ppermute only.
A program may use at most 64 MiB of HBM per device.

```python
import math
import jax
import jax.numpy as jnp
from jax import lax

BLOCK = 256
SBINS = 30
MUBINS = 20
BLK_DEV = 16
CAP = 2
BLOCKS = 512
N_GX = 4
N_WA = 8
DEVICES = 32


def draw_unit_live(key, part):
    units = N_WA * CAP
    key_level, key_full = jax.random.split(jax.random.fold_in(key, 7))
    level = jax.random.randint(key_level, (DEVICES,), 0, 4)
    counts = jnp.right_shift(jnp.full((DEVICES,), units, jnp.int32), level.astype(jnp.int32))
    fullest = jax.random.randint(key_full, (), 0, DEVICES)
    return jnp.where(jnp.arange(DEVICES, dtype=jnp.int32) == fullest, jnp.int32(units), counts).astype(jnp.int32)


def draw_positions(key, part):
    key_centre, key_extent, key_offset = jax.random.split(jax.random.fold_in(key, 11), 3)
    centres = 0.35 + 0.3 * jax.random.uniform(key_centre, (BLOCKS, 3, 1), jnp.float32)
    extent = jnp.exp(jax.random.uniform(key_extent, (BLOCKS, 1, 1), jnp.float32, jnp.log(0.03), jnp.log(0.12)))
    offset = jax.random.uniform(key_offset, (BLOCKS, 3, BLOCK), jnp.float32) - 0.5
    return (centres + extent * offset).astype(jnp.float32)


def set_ends(result, stream_key, low, top_value):
    place = [jax.random.randint(jax.random.fold_in(stream_key, axis), (), 0, length) for axis, length in enumerate(result.shape)]
    widest = result.shape.index(max(result.shape))
    next_to = place[:widest] + [(place[widest] + 1) % result.shape[widest]] + place[widest + 1:]
    return result.at[tuple(place)].set(low).at[tuple(next_to)].set(top_value)


def steps_of(own_key, dims, shards, smallest, largest):
    loudness, own = 1.0, jax.random.fold_in(own_key, 6)
    for axis_at, parts in shards:
        steps = jnp.exp(jax.random.uniform(jax.random.fold_in(own, axis_at), (parts,), jnp.float32, smallest / len(shards), largest / len(shards)))
        loudness = loudness * jnp.repeat(steps, dims[axis_at] // parts).reshape([-1 if axis == axis_at else 1 for axis in range(len(dims))])
    return loudness


def setup_inputs(seed: int = 0) -> dict:
    arg_keys = jax.random.split(jax.random.key(seed), 7)
    return {
        "positions": draw_positions(jax.random.fold_in(arg_keys[6], 71), 0),
        "weights": jnp.clip(jnp.exp(math.log(2.0) - 1.3862944 * jax.random.uniform(arg_keys[1], (BLOCKS, BLOCK), jnp.float32) ** steps_of(arg_keys[1], (BLOCKS, BLOCK), ((0, 32),), -0.2, 0.2)), 0.5, 2.0),
        "block_count": set_ends(jax.random.randint(arg_keys[2], (BLOCKS,), 1, BLOCK + 1), jax.random.fold_in(arg_keys[2], 1), 1, BLOCK).astype(jnp.int32),
        "send_list": set_ends(jax.random.randint(arg_keys[3], (DEVICES, N_WA, CAP), 0, BLK_DEV), jax.random.fold_in(arg_keys[3], 1), 0, BLK_DEV - 1).astype(jnp.int32),
        "unit_pair": jax.vmap(lambda own: jax.random.permutation(own, N_WA * CAP))(jax.random.split(arg_keys[4], DEVICES)).reshape((DEVICES, N_WA * CAP)).astype(jnp.int32),
        "unit_live": draw_unit_live(jax.random.fold_in(arg_keys[6], 71), 0),
    }


reach = 0.5
viewer = (0.5, 0.5, -1.5)

def group_counts(a_pos, a_wgt, b_pos, b_wgt):
    step = reach / SBINS
    diff = a_pos[:, :, :, None] - b_pos[:, :, None, :]
    eye_at = jnp.array(viewer, dtype=jnp.float32)[None, :, None, None]
    middle = 0.5 * (a_pos[:, :, :, None] + b_pos[:, :, None, :]) + eye_at
    square = lax.optimization_barrier(jnp.sum(diff * diff, axis=1))
    dist = jnp.sqrt(square)
    along = jnp.abs(lax.optimization_barrier(jnp.sum(diff * middle, axis=1))) / jnp.sqrt(jnp.maximum(square, step * step) * lax.optimization_barrier(jnp.sum(middle * middle, axis=1)))
    s_mid = jnp.arange(SBINS, dtype=jnp.float32) + 0.5
    m_mid = jnp.arange(MUBINS, dtype=jnp.float32) + 0.5
    s_hat = jnp.maximum(0.0, 1.0 - jnp.abs(dist[:, None] / step - s_mid[None, :, None, None]))
    pair_w = a_wgt[:, :, None] * b_wgt[:, None, :]
    m_hat = jnp.maximum(0.0, 1.0 - jnp.abs(along[:, None] * MUBINS - m_mid[None, :, None, None])) * pair_w[:, None]
    s_low = lax.optimization_barrier(s_hat.astype(jnp.bfloat16)).astype(jnp.float32)
    m_low = lax.optimization_barrier(m_hat.astype(jnp.bfloat16)).astype(jnp.float32)
    return jnp.einsum('gkab,gjab->kj', s_low, m_low, precision=lax.Precision.HIGHEST)

def reference(positions, weights, block_count, send_list, unit_pair, unit_live):
    units = N_WA * CAP
    live = jnp.arange(BLOCK, dtype=jnp.int32)[None, :] < block_count[:, None]
    masked = jnp.where(live, weights, jnp.float32(0.0))
    slab_ix = jnp.arange(N_GX, dtype=jnp.int32)[:, None, None, None]
    src_ix = jnp.arange(N_WA, dtype=jnp.int32)[None, None, :, None]
    listed = jnp.transpose(send_list.reshape(N_GX, N_WA, N_WA, CAP), (0, 2, 1, 3))
    own = ((slab_ix * N_WA + src_ix) * BLK_DEV + listed).astype(jnp.int32).reshape(DEVICES, units)
    below = jnp.roll(own.reshape(N_GX, N_WA, units), 1, axis=0).reshape(DEVICES, units)
    partner = jnp.take_along_axis(below, unit_pair, axis=1)
    active = jnp.arange(units, dtype=jnp.int32)[None, :] < unit_live[:, None]

    def device_counts(item):
        ids_a, ids_b, act = item
        a_pos = positions[ids_a].reshape(units // 4, 4, 3, BLOCK)
        b_pos = positions[ids_b].reshape(units // 4, 4, 3, BLOCK)
        a_wgt = jnp.where(act[:, None], masked[ids_a], jnp.float32(0.0)).reshape(units // 4, 4, BLOCK)
        b_wgt = masked[ids_b].reshape(units // 4, 4, BLOCK)

        def accumulate(total, group):
            return (total + group_counts(*group), None)
        start = jnp.zeros((SBINS, MUBINS), jnp.float32)
        total, _ = lax.scan(accumulate, start, (a_pos, a_wgt, b_pos, b_wgt))
        return total
    per_device = lax.map(device_counts, (own, partner, active))
    scale = 10.0 * SBINS * MUBINS / (N_WA * units * BLOCK * BLOCK)
    slab_counts = lax.optimization_barrier(jnp.sum(per_device.reshape(N_GX, N_WA, SBINS, MUBINS), axis=1)) * scale
    totals = lax.optimization_barrier(jnp.sum(slab_counts, axis=0)) / N_GX
    return (slab_counts, totals)
```

```python
import functools

import jax
import jax.numpy as jnp
from jax import lax
from jax.experimental import pallas as pl
from jax.experimental.pallas import tpu as pltpu
from jax.sharding import PartitionSpec as P

SBINS = 30
MUBINS = 20
REACH = 0.5
STEP = REACH / SBINS
SCALE = 0.5 / STEP
LANES = 128
ROWS = 8
SPAN = 32
SLOTS = 8


def pack_kernel(count_ref, send_ref, pos_ref, wgt_ref, out_ref):
    slots, _, block = out_ref.shape
    per_peer = send_ref.shape[2]
    lane = lax.broadcasted_iota(jnp.int32, (1, block), 1)
    for slot in range(slots):
        src = send_ref[0, slot // per_peer, slot % per_peer]
        count = count_ref[src]
        pos = pos_ref[src]
        wgt = jnp.where(lane < count, wgt_ref[pl.ds(src, 1), :], 0.0)
        mark = jnp.logical_and(lane == block - 1, count < block)
        out_ref[slot, 0:1, :] = jnp.where(mark, count.astype(jnp.float32), pos[0:1])
        out_ref[slot, 1:3, :] = pos[1:3]
        out_ref[slot, 3:4, :] = wgt


def spread(row):
    return jnp.broadcast_to(row, (ROWS, LANES))


def pair_kernel(
    out_scale, live_ref, pair_ref, own_ref, below_ref, out_ref,
    rowf, colf, sep_now, sep_next, ang_next, rowblk, lanblk, wide, steps, *accs
):
    units, _, block = own_ref.shape
    accs = (accs[:SLOTS], accs[SLOTS:])
    live = live_ref[0]
    third = 4.0 * SCALE * SCALE * 3.0

    def features(src_ref, u, b):
        x, y, z, w = (src_ref[u, i:i + 1, :] for i in range(4))
        alive = w > 0.0
        count = jnp.where(alive[:, block - 1:], float(block), x[:, block - 1:])
        x = jnp.where(alive, x, 0.5)
        n = (x - 0.5) * (x + 1.5) + (y - 0.5) * (y + 1.5) + (z - 0.5) * (z - 2.5)
        m = (2.0 * SCALE * SCALE) * n
        feats = jnp.concatenate(
            [SCALE * x, SCALE * y, SCALE * z, (10.0 * SCALE * SCALE) * n, m, w, m + third, w], axis=0
        )
        for half in range(block // LANES):
            rowf[b, half] = feats[:, half * LANES:(half + 1) * LANES]
        colf[b] = feats.T
        return count

    group = 4

    def prepare(i, carry):
        for k in range(group):
            u = i * group + k
            steps[u] = features(own_ref, u, u)[0, 0].astype(jnp.int32)
            wide[u] = features(below_ref, u, units + u)[0, 0].astype(jnp.int32)
        return carry

    lax.fori_loop(0, units // group, prepare, 0)

    def rounds(rows, lanes):
        return jnp.where(lanes > LANES, (rows + 2 * ROWS - 1) // (2 * ROWS), (rows + 4 * ROWS - 1) // (4 * ROWS))

    def plan(u, total):
        other = pair_ref[0, u]
        na, nb = steps[u], wide[other]
        straight, turned = rounds(na, nb), rounds(nb, na)
        turn = turned < straight
        rowblk[u] = jnp.where(turn, units + other, u)
        lanblk[u] = jnp.where(turn, u, units + other)
        n = jnp.where(turn, turned, straight)
        lanblk[units + u] = jnp.where(jnp.where(turn, na, nb) > LANES, 1, 0)
        steps[u] = n
        return total + n

    total = lax.fori_loop(0, live, plan, 0)

    def advance(state):
        u, t = state
        last = t + 1 >= steps[u]
        return jnp.where(last, jnp.minimum(u + 1, live - 1), u), jnp.where(last, 0, t + 1)

    def geometry(state):
        u, t = state
        rb, lb, wd = rowblk[u], lanblk[u], lanblk[units + u]
        sep, ang = [], []
        for j in range(4):
            a0 = pl.multiple_of(jnp.where(wd == 1, t * 16 + 8 * (j // 2), t * 32 + 8 * j), ROWS)
            half = wd * (j % 2)
            col = colf[rb, pl.ds(a0, ROWS), :]
            ax, ay, az, aq, am, aw = (spread(col[:, c:c + 1]) for c in range(6))
            bx, by, bz, bq, bw, bm = (spread(rowf[lb, half, c:c + 1, :]) for c in (0, 1, 2, 3, 5, 6))
            dx, dy, dz = ax - bx, ay - by, az - bz
            square = dx * dx + dy * dy + dz * dz
            y = square * lax.rsqrt(jnp.maximum(square, 1e-12)) + 0.25
            norm = jnp.maximum(square, 0.25) * ((am + bm) - square)
            z = jnp.abs(aq - bq) * lax.rsqrt(norm) + 0.25
            w = aw * bw
            near = jnp.round(y)
            off = jnp.abs(y - near)
            sep.append((jnp.floor(y), near, off, 0.5 - off))
            near = jnp.round(z)
            off = jnp.abs(z - near)
            ang.append((jnp.floor(z), near, off * w, (0.5 - off) * w))
        return sep, ang

    base = lax.broadcasted_iota(jnp.int32, (ROWS, LANES), 0).astype(jnp.float32)
    marks = (base, base + 8.0, base + 1.0, base + 9.0)

    def hats(ref, j, r):
        even, odd, on_even, on_odd = (spread(ref[j, q, r:r + 1, :]) for q in range(4))
        return [
            jnp.where(even == marks[0], on_even, 0.0), jnp.where(even == marks[1], on_even, 0.0),
            jnp.where(odd == marks[2], on_odd, 0.0), jnp.where(odd == marks[3], on_odd, 0.0),
        ]

    def tile(ref, m, r):
        left, right = hats(ref, 2 * m, r), hats(ref, 2 * m + 1, r)
        return jnp.concatenate([jnp.concatenate([a, b], axis=1) for a, b in zip(left, right)], axis=0)

    def put(ref, values):
        for j in range(4):
            for q in range(4):
                ref[j, q] = values[j][q]

    def push():
        for m in range(2):
            rhs = jnp.concatenate([tile(ang_next, m, r) for r in range(SLOTS)], axis=0)
            pltpu.matmul_push_rhs(rhs, staging_register=0, mxu_index=m, transpose=True)

    for m in range(2):
        for r in range(SLOTS):
            pltpu.matmul_pop(accs[m][r])

    first = (jnp.int32(0), jnp.int32(0))
    sep, ang = geometry(first)
    put(sep_now, sep)
    put(ang_next, ang)
    push()
    second = advance(first)
    sep, ang = geometry(second)
    put(sep_next, sep)
    put(ang_next, ang)

    def turn(_, state):
        for r in range(SLOTS):
            for m in range(2):
                pltpu.matmul_acc_lhs(accs[m][r], tile(sep_now, m, r), load_staged_rhs=0 if r == 0 else None)
        push()
        for j in range(4):
            for q in range(4):
                sep_now[j, q] = sep_next[j, q]
        sep, ang = geometry(state)
        put(sep_next, sep)
        put(ang_next, ang)
        return advance(state)

    lax.fori_loop(0, total, turn, advance(second))

    sums = []
    for m in range(2):
        pltpu.matmul_acc_lhs(accs[m][0], jnp.zeros((SPAN, 2 * LANES), jnp.float32), load_staged_rhs=0)
    out = None
    for r in range(SLOTS):
        got = pltpu.matmul_pop(accs[0][r]) + pltpu.matmul_pop(accs[1][r])
        side = r * SPAN // LANES
        got = got[:, side * LANES:(side + 1) * LANES]
        shift = (r * SPAN) % LANES
        if shift:
            got = pltpu.roll(got, LANES - shift, 1)
        out = got if out is None else out + got
    lane = lax.broadcasted_iota(jnp.int32, (SPAN, LANES), 1)
    from_lane = jnp.where(lane % 2 == 0, lane // 2, 16 + lane // 2) % LANES
    out = jnp.take_along_axis(out, from_lane, axis=1) * (4.0 * out_scale)
    half = SBINS // 2
    out_ref[pl.ds(0, half, stride=2), :] = out[:half, :MUBINS]
    out_ref[pl.ds(1, half, stride=2), :] = out[16:16 + half, :MUBINS]


def passed_along(shard, axis, by):
    count = lax.axis_size(axis)
    return lax.ppermute(shard, axis, [(i, (i + by) % count) for i in range(count)])


def swapped(shard, axis, mask):
    return lax.ppermute(shard, axis, [(i, i ^ mask) for i in range(lax.axis_size(axis))])


def per_device(positions, weights, block_count, send_list, unit_pair, unit_live):
    blocks, _, block = positions.shape
    per_peer = send_list.shape[2]
    peers = lax.axis_size("wa")
    units = peers * per_peer
    smem = pl.BlockSpec(memory_space=pltpu.SMEM)
    vmem = pl.BlockSpec(memory_space=pltpu.VMEM)
    slot = jax.ShapeDtypeStruct((units, 4, block), jnp.float32)
    payload = pl.pallas_call(
        pack_kernel, out_shape=slot, in_specs=[smem, smem, vmem, vmem], out_specs=vmem, name="pack"
    )(block_count, send_list, positions, weights)
    own = lax.all_to_all(payload, "wa", split_axis=0, concat_axis=0, tiled=True)
    below = passed_along(own, "gx", 1)
    scale = 10.0 * SBINS * MUBINS / (peers * units * block * block)
    held = pltpu.VMEM((4, 4, ROWS, LANES), jnp.float32)

    def outer(*refs):
        def inner(*accs):
            pair_kernel(scale, *refs, *accs)

        pl.run_scoped(inner, *[pltpu.ACC(m)((SPAN, 2 * LANES), jnp.float32) for m in range(2) for _ in range(SLOTS)])

    total = pl.pallas_call(
        outer,
        out_shape=jax.ShapeDtypeStruct((SBINS, MUBINS), jnp.float32),
        in_specs=[smem, smem, vmem, vmem],
        out_specs=vmem,
        scratch_shapes=[
            pltpu.VMEM((2 * units, block // LANES, 8, LANES), jnp.float32),
            pltpu.VMEM((2 * units, block, 8), jnp.float32),
            held, held, held,
            pltpu.SMEM((units,), jnp.int32),
            pltpu.SMEM((2 * units,), jnp.int32),
            pltpu.SMEM((units,), jnp.int32),
            pltpu.SMEM((units,), jnp.int32),
        ],
        name="pairs",
    )(unit_live, unit_pair, own, below)
    total = total + swapped(total, "wa", 1)
    slab = total
    for mask in range(2, peers, 2):
        slab = slab + swapped(total, "wa", mask)
    whole = slab
    for by in range(1, lax.axis_size("gx")):
        whole = whole + passed_along(slab, "gx", by)
    return (slab[None], whole / lax.axis_size("gx"))


def solution(mesh):
    return jax.shard_map(
        per_device,
        mesh=mesh,
        in_specs=(
            P(("gx", "wa"), None, None),
            P(("gx", "wa"), None),
            P(("gx", "wa")),
            P(("gx", "wa"), None, None),
            P(("gx", "wa"), None),
            P(("gx", "wa")),
        ),
        out_specs=(P("gx", None, None), P()),
        check_vma=False,
    )
```
